32 devices in a mesh: cap: 8 (over y, x, core), tile: 4 (over z).
Axes of the slice: x: 2, y: 2, z: 4, core: 2. Of those that a mesh axis runs over, the one named last changes fastest.
Arguments:
- load: float32 [3, 16, 1536, 128], P(None, 'cap', 'tile'), may hold values from -6 to 6
- previous: float32 [3, 16, 1536, 128], P(None, 'cap', 'tile'), may hold values from -4 to 4
- stress_old: float32 [12, 16, 1536, 128], P(None, 'cap', 'tile'), may hold values from -6 to 6
- shear_modulus: float32 [16, 1536, 128], P('cap', 'tile'), may hold values from 0.5 to 5
- relaxation: float32 [16, 1536, 128], P('cap', 'tile'), may hold values from 0.05 to 2
- density_jump: float32 [16], P('cap'), may hold values from 0.2 to 2
- element_stiffness: float32 [12, 12], replicated, may hold values from -2.9 to 3.4, as said below
- degree_slots: int32 [768], replicated, may hold values from 0 to 767, each once
Outputs:
- displacement: float32 [3, 16, 1536, 128], P(None, 'cap', 'tile')
- stress_new: float32 [12, 16, 1536, 128], P(None, 'cap', 'tile')
- potential_coeffs: float32 [768, 16, 256], P('tile', 'cap')
The draws below stay inside these ranges and needn't reach their ends.
Inputs may be any that keep to these rules, and one draw needn't show every extreme that they name: `element_stiffness`: symmetric positive definite. `degree_slots`: each degree 0 to 767 sits in exactly one slot.
All inputs are finite; a program needn't handle non-finite values.
Results may differ from the reference program's by a relative error of at most 0.00013.
Values sent between devices are 32-bit elements; how exact they have to be, the bound alone decides.
A program may use at most 128 MiB of HBM per device.

```python
import math
import jax
import jax.numpy as jnp
from jax import lax

S = 128
HRING = 1536
LDEG = 768
ITERS = 6
NR = 16


def draw_element_stiffness(key, part):
    factors = jax.random.uniform(key, (12, 12), jnp.float32, -1.7, 1.7)
    return jnp.dot(factors, factors.T) / 12.0 + 0.5 * jnp.eye(12, dtype=jnp.float32)


def steps_of(own_key, extent, pieces, smallest, top_value):
    gain, own = 1.0, jax.random.fold_in(own_key, 6)
    for dim, parts in pieces:
        steps = jnp.exp(jax.random.uniform(jax.random.fold_in(own, dim), (parts,), jnp.float32, smallest / len(pieces), top_value / len(pieces)))
        gain = gain * jnp.repeat(steps, extent[dim] // parts).reshape([-1 if axis == dim else 1 for axis in range(len(extent))])
    return gain


def bell_draw(own_key, dims, width, limit, shards=(), kind=jnp.bfloat16):
    gain = steps_of(own_key, dims, shards, -0.22, 0.18) if shards else 1.0
    drawn = jax.random.normal(own_key, dims, jnp.float32) * width * gain
    return jnp.minimum(jnp.maximum(drawn, -limit), limit).astype(kind)


def setup_inputs(seed: int = 0) -> dict:
    streams_of = jax.random.split(jax.random.key(seed), 9)
    load = bell_draw(streams_of[0], (3, NR, HRING, S), 1.0, 6.0, ((1, 8), (2, 4)), jnp.float32)
    previous = bell_draw(streams_of[1], (3, NR, HRING, S), 0.5, 4.0, ((1, 8), (2, 4)), jnp.float32)
    stress_old = bell_draw(streams_of[2], (12, NR, HRING, S), 1.0, 6.0, ((1, 8), (2, 4)), jnp.float32)
    shear_modulus = jnp.clip(jnp.exp(math.log(5.0) - 2.3025851 * jax.random.uniform(streams_of[3], (NR, HRING, S), jnp.float32) ** steps_of(streams_of[3], (NR, HRING, S), ((0, 8), (1, 4)), -0.2, 0.2)), 0.5, 5.0)
    relaxation = jnp.clip(jnp.exp(math.log(2.0) - 3.6888794 * jax.random.uniform(streams_of[4], (NR, HRING, S), jnp.float32) ** steps_of(streams_of[4], (NR, HRING, S), ((0, 8), (1, 4)), -0.2, 0.2)), 0.05, 2.0)
    density_jump = jnp.clip(jnp.exp(math.log(2.0) - 2.3025851 * jax.random.uniform(streams_of[5], (NR,), jnp.float32) ** steps_of(streams_of[5], (NR,), ((0, 8),), -0.2, 0.2)), 0.2, 2.0)
    element_stiffness = draw_element_stiffness(jax.random.fold_in(streams_of[8], 71), 0)
    degree_slots = jax.random.permutation(streams_of[7], LDEG).astype(jnp.int32)
    return dict(load=load, previous=previous, stress_old=stress_old, shear_modulus=shear_modulus, relaxation=relaxation, density_jump=density_jump, element_stiffness=element_stiffness, degree_slots=degree_slots)


precise = lax.Precision.HIGHEST
rotation_gain = 2.0
gravity_gain = 0.2

def radius_rows(offset, amount, layers):
    positions = (offset + jnp.arange(amount, dtype=jnp.int32)).astype(jnp.float32)
    return 1.0 - 0.45 * (positions + 0.5) / layers

def cycle_basis(degrees, columns):
    windings = degrees[:, None] * columns[None, :] % HRING
    angles = windings.astype(jnp.float32) * (2.0 * math.pi / HRING)
    return (jnp.cos(angles), jnp.sin(angles))

def green_kernel(degrees, target_radius, source_radius):
    degree_float = degrees.astype(jnp.float32)
    distance = jnp.abs(jnp.log(target_radius)[:, None] - jnp.log(source_radius)[None, :])
    return jnp.exp(-degree_float[:, None, None] * distance[None]) / jnp.sqrt(2.0 * degree_float + 1.0)[:, None, None]

def rotation_term(degrees, radius_list, moment):
    selector = (degrees == 2).astype(jnp.float32)
    return rotation_gain * selector[:, None, None] * (radius_list ** 2)[None, :, None] * moment[:, None, :]

def corner_values(nodal_field):
    padded = jnp.concatenate([nodal_field, jnp.zeros_like(nodal_field[:, :1])], axis=1)
    shallow = padded[:, :-1]
    deeper = padded[:, 1:]
    stacked = jnp.stack([shallow, jnp.roll(shallow, -1, axis=2), deeper, jnp.roll(deeper, -1, axis=2)], axis=1)
    return stacked.reshape((12,) + nodal_field.shape[1:])

def assemble(forces):
    grouped = forces.reshape((3, 4) + forces.shape[1:])
    shallow = grouped[:, 0] + jnp.roll(grouped[:, 1], 1, axis=2)
    deeper = grouped[:, 2] + jnp.roll(grouped[:, 3], 1, axis=2)
    moved = jnp.concatenate([jnp.zeros_like(deeper[:, :1]), deeper[:, :-1]], axis=1)
    return shallow + moved

def element_forces(nodal_field, stiffness, effective):
    return effective[None] * jnp.einsum('ab,brhs->arhs', stiffness, corner_values(nodal_field), precision=precise)

def reference(load, previous, stress_old, shear_modulus, relaxation, density_jump, element_stiffness, degree_slots):
    effective = shear_modulus / (1.0 + 0.5 * relaxation)
    carried_share = relaxation / (1.0 + 0.5 * relaxation)
    retained = (1.0 - 0.5 * relaxation) / (1.0 + 0.5 * relaxation)
    radius_all = radius_rows(0, NR, NR)
    columns = jnp.arange(HRING, dtype=jnp.int32)
    cosine, sine_table = cycle_basis(degree_slots, columns)
    weighted = previous[0] * density_jump[:, None, None]
    normalizer = math.sqrt(2.0 / HRING)
    first_half = jnp.einsum('kh,rhs->krs', cosine, weighted, precision=precise)
    second_half = jnp.einsum('kh,rhs->krs', sine_table, weighted, precision=precise)
    coefficients = jnp.concatenate([first_half, second_half], axis=2) * normalizer
    kernel = green_kernel(degree_slots, radius_all, radius_all)
    moment = jnp.einsum('j,kjs->ks', radius_all ** 4 / NR, coefficients, precision=precise)
    potential = jnp.einsum('kij,kjs->kis', kernel, coefficients, precision=precise)
    potential = potential + rotation_term(degree_slots, radius_all, moment)
    potential_field = jnp.einsum('krs,kh->rhs', potential[:, :, :S], cosine, precision=precise)
    potential_field = potential_field + jnp.einsum('krs,kh->rhs', potential[:, :, S:], sine_table, precision=precise)
    gravity_force = gravity_gain * density_jump[:, None, None] * potential_field
    right_side = load + assemble(carried_share[None] * stress_old)
    right_side = right_side + jnp.concatenate([gravity_force[None], jnp.zeros_like(load[1:])], axis=0)

    def operate(vector):
        return assemble(element_forces(vector, element_stiffness, effective))
    residual = right_side - operate(previous)
    norm_start = jnp.sum(residual * residual)

    def iterate(counter, carry_state):
        solution, residual, direction, norm_now = carry_state
        applied = operate(direction)
        step_size = norm_now / jnp.sum(direction * applied)
        solution = solution + step_size * direction
        residual = residual - step_size * applied
        norm_next = jnp.sum(residual * residual)
        direction = residual + norm_next / norm_now * direction
        return (solution, residual, direction, norm_next)
    solution = lax.fori_loop(0, ITERS, iterate, (previous, residual, residual, norm_start))[0]
    stress_new = retained[None] * stress_old + element_forces(solution, element_stiffness, effective)
    return (solution, stress_new, potential)
```

```python
import math

import jax
import jax.numpy as jnp
from jax import lax
from jax.experimental import pallas as pl
from jax.experimental.pallas import tpu as pltpu
from jax.sharding import PartitionSpec as P

HRING = 1536
LDEG = 768
ITERS = 6


precise = lax.Precision.HIGHEST
rotation_gain = 2.0
gravity_gain = 0.2


def from_behind(block, axis, distance):
    devices = range(lax.axis_size(axis))
    route = [((i - distance) % len(devices), i) for i in devices]
    return lax.ppermute(block, axis, route)


def from_behind_2(block, axis, distance):
    devices = range(lax.axis_size(axis))
    route = [(i - distance, i) for i in devices if i - distance in devices]
    return lax.ppermute(block, axis, route)


def radius_rows(offset, amount, layers):
    positions = (offset + jnp.arange(amount, dtype=jnp.int32)).astype(jnp.float32)
    return 1.0 - 0.45 * (positions + 0.5) / layers


def cycle_basis(degrees, columns):
    windings = degrees[:, None] * columns[None, :] % HRING
    angles = windings.astype(jnp.float32) * (2.0 * math.pi / HRING)
    return (jnp.cos(angles), jnp.sin(angles))


def green_kernel(degrees, target_radius, source_radius):
    degree_float = degrees.astype(jnp.float32)
    distance = jnp.abs(jnp.log(target_radius)[:, None] - jnp.log(source_radius)[None, :])
    return (
        jnp.exp(-degree_float[:, None, None] * distance[None])
        / jnp.sqrt(2.0 * degree_float + 1.0)[:, None, None]
    )


def rotation_term(degrees, radius_list, moment):
    selector = (degrees == 2).astype(jnp.float32)
    return (
        rotation_gain
        * selector[:, None, None]
        * (radius_list**2)[None, :, None]
        * moment[:, None, :]
    )


def place_corner(portion, top_pad, left_pad):
    return jnp.pad(portion, ((0, 0), (top_pad, 1 - top_pad), (left_pad, 1 - left_pad), (0, 0)))


def fold_forces(forces):
    grouped = forces.reshape((3, 4) + forces.shape[1:])
    row_count = forces.shape[1]
    col_count = forces.shape[2]
    padded_sum = place_corner(grouped[:, 0], 0, 0) + place_corner(grouped[:, 1], 0, 1)
    padded_sum = padded_sum + place_corner(grouped[:, 2], 1, 0) + place_corner(grouped[:, 3], 1, 1)
    spill_column = from_behind(padded_sum[:, :, col_count:, :], "tile", 1)
    interior = padded_sum[:, :, :col_count, :] + jnp.pad(
        spill_column, ((0, 0), (0, 0), (0, col_count - 1), (0, 0))
    )
    spill_row = from_behind_2(interior[:, row_count:], "cap", 1)
    return interior[:, :row_count] + jnp.pad(
        spill_row, ((0, 0), (0, row_count - 1), (0, 0), (0, 0))
    )


CHUNK = 16
MESH = pl.DeviceIdType.MESH
PAIRS = ((0, 0), (0, 1), (0, 2), (1, 1), (1, 2), (2, 2))
BAND = 42


def remote(src, dst, send, recv, to_cap, to_tile):
    return pltpu.make_async_remote_copy(
        src_ref=src, dst_ref=dst, send_sem=send, recv_sem=recv,
        device_id=(to_cap, to_tile), device_id_type=MESH,
    )


def build_band(k_ref, eff, band, row, width):
    def entry(c, q, d, p):
        return k_ref[4 * c + q, 4 * d + p]

    half = width // 2
    for start in (0, half):
        here = pl.ds(start, half)
        ahead = eff[row, pl.ds(start + 8, half), :]
        behind = eff[row, pl.ds(start + 7, half), :]
        up_ahead = eff[row - 1, pl.ds(start + 8, half), :]
        up_behind = eff[row - 1, pl.ds(start + 7, half), :]
        for n, (c, d) in enumerate(PAIRS):
            band[n, row, here, :] = (
                ahead * entry(c, 0, d, 0) + behind * entry(c, 1, d, 1)
                + up_ahead * entry(c, 2, d, 2) + up_behind * entry(c, 3, d, 3)
            )
        for c in range(3):
            for d in range(3):
                n = 3 * c + d
                band[6 + n, row, here, :] = (
                    ahead * entry(c, 0, d, 1) + up_ahead * entry(c, 2, d, 3)
                )
                band[15 + n, row, here, :] = (
                    ahead * entry(c, 0, d, 2) + behind * entry(c, 1, d, 3)
                )
                band[24 + n, row, here, :] = ahead * entry(c, 0, d, 3)
                band[33 + n, row, here, :] = behind * entry(c, 1, d, 2)


def band_rows(band, field, row, start, chunk, count):
    values = {}

    def value(c, i, shift):
        if (c, i, shift) not in values:
            values[c, i, shift] = field[c, row + i, pl.ds(start + shift, chunk), :]
        return values[c, i, shift]

    def coupling(n, i, shift=0):
        return band[n, row + i, pl.ds(start + shift, chunk), :]

    results = []
    for i in range(count):
        outs = []
        for c in range(3):
            terms = []
            for d in range(3):
                n, m = 3 * c + d, 3 * d + c
                pair = PAIRS.index((min(c, d), max(c, d)))
                terms += [
                    coupling(pair, i) * value(d, i, 0),
                    coupling(6 + n, i) * value(d, i, 1),
                    coupling(6 + m, i, -1) * value(d, i, -1),
                    coupling(15 + n, i) * value(d, i + 1, 0),
                    coupling(15 + m, i - 1) * value(d, i - 1, 0),
                    coupling(24 + n, i) * value(d, i + 1, 1),
                    coupling(24 + m, i - 1, -1) * value(d, i - 1, -1),
                    coupling(33 + n, i) * value(d, i + 1, -1),
                    coupling(33 + m, i - 1, 1) * value(d, i - 1, 1),
                ]
            total = terms[0]
            for term in terms[1:]:
                total = total + term
            outs.append(total)
        results.append(outs)
    return results


def solve_kernel(
    k_ref, prev_ref, rhs_ref, eff_ref, out_ref,
    prev_all, rhs_all, eff_all, eff_pad, band, res, image, adir, direc, sol,
    edge_out, edge_in, eff_edge_out, eff_edge_in, sums, stat, back, rim_out, rim_in,
    in_send, in_recv, own_sem, edge_send, edge_recv, sum_send, sum_recv,
    back_send, back_recv, rim_send, rim_recv,
):
    caps = lax.axis_size("cap")
    tiles = lax.axis_size("tile")
    cap = lax.axis_index("cap")
    tile = lax.axis_index("tile")
    devices = caps * tiles
    me = cap * tiles + tile
    rows = prev_ref.shape[1]
    width = prev_ref.shape[3]
    sections = prev_ref.shape[4]
    layers = rows * caps
    chunk = 8 if width % 8 == 0 else width
    chunks = width // chunk
    inner = pl.ds(8, width)
    own_rows = pl.ds(rows * cap, rows)

    def device(d):
        other = lax.rem(me + d, devices)
        return lax.div(other, tiles), lax.rem(other, tiles)

    barrier = pltpu.get_barrier_semaphore()

    def greet(d, carry):
        pl.semaphore_signal(barrier, inc=1, device_id=device(d), device_id_type=MESH)
        return carry

    lax.fori_loop(1, devices, greet, 0)
    pl.semaphore_wait(barrier, devices - 1)

    exchanged = (
        (eff_ref, eff_all, lambda ref, b: ref.at[:, b], lambda ref: ref.at[own_rows]),
        (prev_ref, prev_all, lambda ref, b: ref.at[:, :, b], lambda ref: ref.at[:, own_rows]),
        (rhs_ref, rhs_all, lambda ref, b: ref.at[:, :, b], lambda ref: ref.at[:, own_rows]),
    )
    arrivals = []
    for n, (src, dst, part, place) in enumerate(exchanged):
        copies = [
            remote(
                part(src, lax.rem(cap + d, caps)), place(dst),
                in_send.at[n, d - 1], in_recv.at[n, d - 1], lax.rem(cap + d, caps), tile,
            )
            for d in range(1, caps)
        ]
        copies.append(pltpu.make_async_copy(part(src, cap), place(dst), own_sem.at[n]))
        for copy in copies:
            copy.start()
        arrivals.append(copies)

    place_now = cap + caps * tile
    total_places = caps * tiles
    after = lax.rem(place_now + 1, total_places)
    before = lax.rem(place_now + total_places - 1, total_places)

    def edge_copies(kind):
        right = remote(
            edge_out.at[kind, 1], edge_in.at[kind, 0], edge_send.at[kind, 0],
            edge_recv.at[kind, 0], lax.rem(after, caps), lax.div(after, caps),
        )
        left = remote(
            edge_out.at[kind, 0], edge_in.at[kind, 1], edge_send.at[kind, 1],
            edge_recv.at[kind, 1], lax.rem(before, caps), lax.div(before, caps),
        )
        return right, left

    def insert_edges(field, kind):
        for c in range(3):
            for r in range(layers):
                field[c, r + 1, pl.ds(7, 1), :] = edge_in[kind, 0, c, pl.ds(r, 1), :]
                field[c, r + 1, pl.ds(8 + width, 1), :] = edge_in[kind, 1, c, pl.ds(r, 1), :]

    blank = jnp.zeros((width + 16, sections), jnp.float32)
    for c in range(3):
        res[c, 0] = blank
        res[c, layers + 1] = blank
    eff_pad[0] = jnp.zeros(eff_pad.shape[1:], jnp.float32)

    def clear(r, carry):
        for c in range(3):
            adir[c, r + 1] = blank
            direc[c, r] = jnp.zeros((width, sections), jnp.float32)
        eff_pad[r + 1] = jnp.zeros(eff_pad.shape[1:], jnp.float32)
        return carry

    lax.fori_loop(0, layers, clear, 0)
    stat[...] = jnp.ones(stat.shape, jnp.float32)
    for n in range(BAND):
        band[n, 0] = blank
    for c in range(3):
        sol[c, layers] = jnp.zeros((width, sections), jnp.float32)

    for copy in arrivals[0]:
        copy.wait()
    for r in range(layers):
        eff_edge_out[pl.ds(r, 1), :] = eff_all[r, pl.ds(width - 1, 1), :]
    eff_copy = remote(
        eff_edge_out, eff_edge_in, edge_send.at[4, 0], edge_recv.at[4, 0],
        lax.rem(after, caps), lax.div(after, caps),
    )
    eff_copy.start()
    for copy in arrivals[1]:
        copy.wait()
    for r in range(layers):
        for c in range(3):
            edge_out[2, 0, c, pl.ds(r, 1), :] = prev_all[c, r, pl.ds(0, 1), :]
            edge_out[2, 1, c, pl.ds(r, 1), :] = prev_all[c, r, pl.ds(width - 1, 1), :]
    first_edges = edge_copies(2)
    for copy in first_edges:
        copy.start()

    def settle(r, carry):
        for c in range(3):
            here = prev_all[c, r]
            res[c, r + 1, inner, :] = here
            sol[c, r] = here
        eff_pad[r + 1, pl.ds(16, width), :] = eff_all[r]
        return carry

    lax.fori_loop(0, layers, settle, 0)
    eff_copy.wait()
    for r in range(layers):
        eff_pad[r + 1, pl.ds(15, 1), :] = eff_edge_in[pl.ds(r, 1), :]

    def couple(r, carry):
        build_band(k_ref, eff_pad, band, r + 1, width + 16)
        return carry

    lax.fori_loop(0, layers, couple, 0)
    for copy in first_edges:
        copy.wait()
    insert_edges(res, 2)

    def operate(field, emit, carry):
        def step(pair, inner_carry):
            row = 2 * pair + 1
            for k in range(chunks):
                start = 8 + k * chunk
                for i, outs in enumerate(band_rows(band, field, row, start, chunk, 2)):
                    inner_carry = emit(row + i, k, start, outs, inner_carry)
            return inner_carry

        return lax.fori_loop(0, layers // 2, step, carry)

    def edge_rows(kind, row, k, outs):
        for c in range(3):
            if k == 0:
                edge_out[kind, 0, c, pl.ds(row - 1, 1), :] = outs[c][:1]
            if k == chunks - 1:
                edge_out[kind, 1, c, pl.ds(row - 1, 1), :] = outs[c][chunk - 1 :]

    for copy in arrivals[2]:
        copy.wait()

    def start_residual(row, k, start, outs, carry):
        here = [
            rhs_all[c, row - 1, pl.ds(start - 8, chunk), :] - outs[c] for c in range(3)
        ]
        for c in range(3):
            image[c, row, pl.ds(start, chunk), :] = here[c]
        edge_rows(3, row, k, here)
        return carry

    operate(res, start_residual, 0)
    second_edges = edge_copies(3)
    for copy in second_edges:
        copy.start()

    def adopt(r, carry):
        for c in range(3):
            res[c, r + 1, inner, :] = image[c, r + 1, inner, :]
        return carry

    lax.fori_loop(0, layers, adopt, 0)
    for copy in second_edges:
        copy.wait()
    insert_edges(res, 3)

    def sum_copy(par, d):
        to_cap, to_tile = device(d)
        return remote(
            sums.at[par, me], sums.at[par, me], sum_send.at[par, d - 1],
            sum_recv.at[par, d - 1], to_cap, to_tile,
        )

    def iterate(k, last):
        par = lax.rem(k, 2)

        def apply_emit(row, j, start, outs, carry):
            norm, product = carry
            for c in range(3):
                here = res[c, row, pl.ds(start, chunk), :]
                if not last:
                    image[c, row, pl.ds(start, chunk), :] = outs[c]
                norm = norm + here * here
                product = product + here * outs[c]
            if not last:
                edge_rows(par, row, j, outs)
            return norm, product

        zero = jnp.zeros((chunk, sections), jnp.float32)
        norm, product = operate(res, apply_emit, (zero, zero))
        sums[par, me, pl.ds(0, 1), :] = jnp.sum(norm, axis=0, keepdims=True)
        sums[par, me, pl.ds(1, 1), :] = jnp.sum(product, axis=0, keepdims=True)

        def begin(d, carry):
            sum_copy(par, d).start()
            return carry

        lax.fori_loop(1, devices, begin, 0)
        if not last:
            for copy in edge_copies(par):
                copy.start()

        def finish(d, carry):
            sum_copy(par, d).wait()
            return carry

        if not last:
            for copy in edge_copies(par):
                copy.wait()
            insert_edges(image, par)
        lax.fori_loop(1, devices, finish, 0)
        joined = sums[par, 0]
        for n in range(1, devices):
            joined = joined + sums[par, n]
        both = jnp.broadcast_to(jnp.sum(joined, axis=1, keepdims=True), joined.shape)
        norm_next = both[:1]
        growth = jnp.where(k == 0, 0.0, norm_next / stat[0])
        size = norm_next / (both[1:] - growth * norm_next / stat[1])
        stat[0] = norm_next
        stat[1] = size

        def update(r, carry):
            for c in range(3):
                along = res[c, r + 1, inner, :] + growth * direc[c, r]
                sol[c, r] = sol[c, r] + size * along
                if not last:
                    direc[c, r] = along
                    whole = image[c, r + 1] + growth * adir[c, r + 1]
                    adir[c, r + 1] = whole
                    res[c, r + 1] = res[c, r + 1] - size * whole
            return carry

        lax.fori_loop(0, layers, update, 0)

    def turn(k, carry):
        iterate(k, False)
        return carry

    lax.fori_loop(0, ITERS - 1, turn, 0)
    iterate(jnp.int32(ITERS - 1), True)

    returns = [
        remote(
            sol.at[:, pl.ds(rows * lax.rem(cap + d, caps), rows + 1)], back.at[:, :, cap],
            back_send.at[d - 1], back_recv.at[d - 1], lax.rem(cap + d, caps), tile,
        )
        for d in range(1, caps)
    ]
    for copy in returns:
        copy.start()

    for r in range(layers + 1):
        for c in range(3):
            rim_out[r, pl.ds(c, 1), :] = sol[c, r, pl.ds(0, 1), :]
    behind_tile = lax.rem(tile + tiles - 1, tiles)

    def rim_copy(to):
        return remote(
            rim_out.at[pl.ds(rows * to, rows + 1)], rim_in, rim_send.at[to], rim_recv,
            to, behind_tile,
        )

    @pl.when(cap == 0)
    def _():
        for to in range(caps):
            rim_copy(to).start()

    own = pl.ds(rows * cap, rows + 1)
    for c in range(3):
        back[c, :, cap] = sol[c, own]
    for copy in returns:
        copy.wait()
    rim_copy(0).wait_recv()

    @pl.when(cap == 0)
    def _():
        for to in range(caps):
            rim_copy(to).wait_send()

    for c in range(3):
        for r in range(rows + 1):
            for b in range(caps):
                out_ref[c, r, pl.ds(b * width, width), :] = back[c, r, b]
            out_ref[c, r, pl.ds(caps * width, 1), :] = rim_in[r, pl.ds(c, 1), :]


def solve(stiffness, previous, right_side, effective):
    caps = lax.axis_size("cap")
    tiles = lax.axis_size("tile")
    _, rows, cols, sections = previous.shape
    width = cols // caps
    layers = rows * caps
    devices = caps * tiles
    split = (3, rows, caps, width, sections)
    dma = pltpu.SemaphoreType.DMA
    f32 = jnp.float32
    padded = pltpu.VMEM((3, layers + 2, width + 16, sections), f32)
    plain = pltpu.VMEM((3, layers, width, sections), f32)
    return pl.pallas_call(
        solve_kernel,
        out_shape=jax.ShapeDtypeStruct((3, rows + 1, cols + 8, sections), f32),
        in_specs=[pl.BlockSpec(memory_space=pltpu.SMEM)]
        + [pl.BlockSpec(memory_space=pl.ANY)] * 3,
        out_specs=pl.BlockSpec(memory_space=pltpu.VMEM),
        scratch_shapes=[
            plain,
            plain,
            pltpu.VMEM((layers, width, sections), f32),
            pltpu.VMEM((layers + 1, width + 32, sections), f32),
            pltpu.VMEM((BAND, layers + 1, width + 16, sections), f32),
            padded,
            padded,
            padded,
            plain,
            pltpu.VMEM((3, layers + 1, width, sections), f32),
            pltpu.VMEM((4, 2, 3, layers, sections), f32),
            pltpu.VMEM((4, 2, 3, layers, sections), f32),
            pltpu.VMEM((layers, sections), f32),
            pltpu.VMEM((layers, sections), f32),
            pltpu.VMEM((2, devices, 2, sections), f32),
            pltpu.VMEM((2, 1, sections), f32),
            pltpu.VMEM((3, rows + 1, caps, width, sections), f32),
            pltpu.VMEM((layers + 1, 3, sections), f32),
            pltpu.VMEM((rows + 1, 3, sections), f32),
            dma((3, caps - 1)),
            dma((3, caps - 1)),
            dma((3,)),
            dma((5, 2)),
            dma((5, 2)),
            dma((2, devices - 1)),
            dma((2, devices - 1)),
            dma((caps - 1,)),
            dma((caps - 1,)),
            dma((caps,)),
            dma,
        ],
        compiler_params=pltpu.CompilerParams(
            collective_id=0, has_side_effects=True, vmem_limit_bytes=60 * 1024 * 1024
        ),
        name="cg_solve",
    )(
        stiffness,
        previous.reshape(split),
        right_side.reshape(split),
        effective.reshape(split[1:]),
    )


def pair_forces(k_ref, corners, eff, c, q):
    total = k_ref[4 * c + q, 0] * corners[0]
    for b in range(1, 12):
        total = total + k_ref[4 * c + q, b] * corners[b]
    return eff * total


def stress_kernel(k_ref, sol_ref, shear_ref, relax_ref, old_ref, new_ref, disp_ref):
    e = pl.program_id(0)
    width = old_ref.shape[2]
    base = pl.program_id(1) * width

    def step(i, carry):
        here = pl.ds(pl.multiple_of(i * CHUNK, CHUNK), CHUNK)
        p = pl.multiple_of(base + i * CHUNK, 8)
        corners = [
            sol_ref[c, row, pl.ds(p + shift, CHUNK), :]
            for c in range(3)
            for row in (e, e + 1)
            for shift in (0, 1)
        ]
        relaxation = relax_ref[0, here, :]
        inverse = 1.0 / (1.0 + 0.5 * relaxation)
        eff = shear_ref[0, here, :] * inverse
        retained = (1.0 - 0.5 * relaxation) * inverse
        for c in range(3):
            disp_ref[c, 0, here, :] = corners[4 * c]
            for q in range(4):
                new_ref[4 * c + q, 0, here, :] = retained * old_ref[
                    4 * c + q, 0, here, :
                ] + pair_forces(k_ref, corners, eff, c, q)
        return carry

    lax.fori_loop(0, width // CHUNK, step, 0)


def stress_update(stiffness, sol_ext, shear_modulus, relaxation, stress_old):
    _, rows, cols, sections = stress_old.shape
    width = cols // 4
    block = pl.BlockSpec((12, 1, width, sections), lambda r, j: (0, r, j, 0))
    moduli = pl.BlockSpec((1, width, sections), lambda r, j: (r, j, 0))
    f32 = jnp.float32
    return pl.pallas_call(
        stress_kernel,
        grid=(rows, cols // width),
        out_shape=(
            jax.ShapeDtypeStruct(stress_old.shape, f32),
            jax.ShapeDtypeStruct((3, rows, cols, sections), f32),
        ),
        in_specs=[
            pl.BlockSpec(memory_space=pltpu.SMEM),
            pl.BlockSpec(sol_ext.shape, lambda r, j: (0, 0, 0, 0)),
            moduli,
            moduli,
            block,
        ],
        out_specs=(block, pl.BlockSpec((3, 1, width, sections), lambda r, j: (0, r, j, 0))),
        compiler_params=pltpu.CompilerParams(vmem_limit_bytes=32 * 1024 * 1024),
        name="stress_update",
    )(stiffness, sol_ext, shear_modulus, relaxation, stress_old)


def scatter_sum(values, tile_place, slot_count):
    tiles = lax.axis_size("tile")

    def share(owner):
        return lax.dynamic_slice_in_dim(values, owner * slot_count, slot_count, 0)

    total = share(tile_place)
    for d in range(1, tiles):
        total = total + from_behind(share((tile_place + d) % tiles), "tile", d)
    return total


def body(
    load,
    previous,
    stress_old,
    shear_modulus,
    relaxation,
    density_jump,
    element_stiffness,
    degree_slots,
):
    effective = shear_modulus / (1.0 + 0.5 * relaxation)
    carried_share = relaxation / (1.0 + 0.5 * relaxation)
    sections = load.shape[3]
    depth_rows = load.shape[1]
    cycle_cols = load.shape[2]
    cap_count = lax.axis_size("cap")
    tile_count = lax.axis_size("tile")
    layers = depth_rows * cap_count
    slot_count = LDEG // tile_count
    cap_place = lax.axis_index("cap")
    tile_place = lax.axis_index("tile")
    columns = tile_place * cycle_cols + jnp.arange(cycle_cols, dtype=jnp.int32)
    weighted = previous[0] * density_jump[:, None, None]
    normalizer = math.sqrt(2.0 / HRING)
    residual = fold_forces(carried_share[None] * stress_old) + load
    degrees = degree_slots
    cosine, sine_table = cycle_basis(degrees, columns)
    first_half = jnp.einsum("kh,rhs->krs", cosine, weighted, precision=precise)
    second_half = jnp.einsum("kh,rhs->krs", sine_table, weighted, precision=precise)
    coefficients = scatter_sum(
        jnp.concatenate([first_half, second_half], axis=2) * normalizer, tile_place, slot_count
    )
    own_degrees = lax.dynamic_slice_in_dim(degree_slots, tile_place * slot_count, slot_count, 0)
    own_radius = radius_rows(cap_place * depth_rows, depth_rows, layers)
    portion = lax.all_gather(coefficients, "cap", axis=1, tiled=True)
    source_radius = radius_rows(jnp.int32(0), portion.shape[1], layers)
    kernel = green_kernel(own_degrees, own_radius, source_radius)
    potential = jnp.einsum("kij,kjs->kis", kernel, portion, precision=precise)
    moment = jnp.einsum("j,kjs->ks", source_radius**4 / layers, portion, precision=precise)
    potential, moment = (potential, moment)
    potential = potential + rotation_term(own_degrees, own_radius, moment)
    portion = lax.all_gather(potential, "tile", axis=0, tiled=True)
    degrees = degree_slots
    cosine, sine_table = cycle_basis(degrees, columns)
    running = jnp.einsum("krs,kh->rhs", portion[:, :, :sections], cosine, precision=precise)
    surface_field = running + jnp.einsum(
        "krs,kh->rhs", portion[:, :, sections:], sine_table, precision=precise
    )
    gravity_force = gravity_gain * density_jump[:, None, None] * surface_field
    residual = residual + jnp.concatenate([gravity_force[None], jnp.zeros_like(load[1:])], axis=0)
    sol_ext = solve(element_stiffness, previous, residual, effective)
    stress_new, solution = stress_update(
        element_stiffness, sol_ext, shear_modulus, relaxation, stress_old
    )
    return (solution, stress_new, potential)


def solution(mesh):
    placed = (
        P(None, "cap", "tile", None),
        P(None, "cap", "tile", None),
        P(None, "cap", "tile", None),
        P("cap", "tile", None),
        P("cap", "tile", None),
        P("cap"),
        P(),
        P(),
    )
    return jax.shard_map(
        body,
        mesh=mesh,
        in_specs=placed,
        out_specs=(
            P(None, "cap", "tile", None),
            P(None, "cap", "tile", None),
            P("tile", "cap", None),
        ),
        check_vma=False,
    )
```
